32 devices in a mesh: snap: 2 (over y), row: 8 (over z, x), col: 2 (over core).
Axes of the slice: x: 2, y: 2, z: 4, core: 2. Of those that a mesh axis runs over, the one named last changes fastest.
Arguments:
- density: bfloat16 [8192, 1024], P(('snap', 'row'), 'col'), parts along dimension 0, may hold values from -0.5 to 2
- pattern: int32 [256, 32], P(('snap', 'row'), 'col'), parts along dimension 0, may hold values 0 or 1
- filter_mask: int32 [256, 32], P(('snap', 'row')), parts along dimension 0, may hold values 0 or 1
Outputs:
- purified: bfloat16 [8192, 1024], P(('snap', 'row'), 'col'), parts along dimension 0
- traces: float32 [4], P('snap'), parts along dimension 0
The draws below stay inside these ranges and needn't reach their ends.
There are 2 independent parts, one for each index of `snap`. The reference program is written for one: setup_inputs(seed, part) draws one part's arguments, and reference() takes and returns one part's arrays. A program takes and returns all parts, laid end to end along the dimension named above; each array names one. Nothing has to cross between parts.
All inputs are finite; a program needn't handle non-finite values. No bound on the sum of `pattern` or of `filter_mask` on one device may be relied on, other than what follows from the above.
Results may differ from the reference program's by a relative error of at most 0.006.
Values may be sent and summed in bfloat16 or wider, within the bound.
A program may use at most 64 MiB of HBM per device.

```python
import jax
import jax.numpy as jnp
from jax import lax

BLK = 32
S = 32
H = 16
NB = 128
ORDER = 4096


def draw_density(key, part):
    keys = jax.random.split(jax.random.fold_in(key, 11), 2)
    width = S * BLK
    sigma = 0.9 / width ** 0.5
    row_index = jnp.arange(ORDER, dtype=jnp.int32)
    offdiag = jnp.clip(jax.random.normal(keys[0], (ORDER, width), jnp.float32), -4.5, 4.5) * sigma
    rising = 0.3 + 0.6 * row_index.astype(jnp.float32) / ORDER
    occupied = jax.random.uniform(keys[1], (ORDER,), jnp.float32, 0.5, 1.5) * rising
    column_index = jnp.arange(width, dtype=jnp.int32)
    on_diagonal = column_index[None, :] == (H * BLK + row_index % BLK)[:, None]
    values = offdiag + jnp.where(on_diagonal, occupied[:, None], 0.0)
    return values.astype(jnp.bfloat16)


def place_ends(drawn, stream_key, smallest, top_value):
    longest = drawn.shape.index(max(drawn.shape))
    spots = []
    for shift in (0, 1):
        where = [jax.random.randint(jax.random.fold_in(stream_key, axis), (), 0, length) for axis, length in enumerate(drawn.shape)]
        where[longest] = (where[longest] + shift) % drawn.shape[longest]
        spots.append(tuple(where))
    return drawn.at[spots[0]].set(smallest).at[spots[1]].set(top_value)


def setup_inputs(seed: int = 0, part: int = 0) -> dict:
    streams_of = jax.random.split(jax.random.key(seed), 4)
    part_splits = jax.random.split(jax.random.fold_in(streams_of[3], part), 4)
    return {
        "density": draw_density(jax.random.fold_in(jax.random.fold_in(streams_of[3], part), 71), part),
        "pattern": place_ends((jax.random.randint(part_splits[1], (NB, S), 0, 4) < 3).astype(jnp.int32), jax.random.fold_in(part_splits[1], 1), 0, 1),
        "filter_mask": place_ends((jax.random.randint(part_splits[2], (NB, S), 0, 8) < 7).astype(jnp.int32), jax.random.fold_in(part_splits[2], 1), 0, 1),
    }


def valid_slots(row_total, slot_count, half_band):
    row_index = jnp.arange(row_total, dtype=jnp.int32)
    slot_index = jnp.arange(slot_count, dtype=jnp.int32)
    column_index = row_index[:, None] + slot_index[None, :] - half_band
    return ((column_index >= 0) & (column_index < row_total)).astype(jnp.int32)


def expand_mask(values, keep_mask):
    block_rows = keep_mask.shape[0]
    slot_count = keep_mask.shape[1]
    blocks = values.reshape(block_rows, BLK, slot_count, BLK)
    blocks = blocks * keep_mask.astype(values.dtype)[:, None, :, None]
    return blocks.reshape(block_rows * BLK, slot_count * BLK)


def shift_slots(segment, moved):
    height = segment.shape[0]
    if moved > 0:
        return jnp.concatenate([jnp.zeros((height, moved * BLK), segment.dtype), segment[:, : segment.shape[1] - moved * BLK]], 1)
    if moved < 0:
        return jnp.concatenate([segment[:, -moved * BLK:], jnp.zeros((height, -moved * BLK), segment.dtype)], 1)
    return segment


def band_product(left, right):
    group_rows = 8 if NB % 8 == 0 else 2
    extended = jnp.pad(right, ((H * BLK, H * BLK), (0, 0)))

    def one_group(group):
        first = group * group_rows
        stacked = []
        for offset in range(S):
            segment = lax.dynamic_slice_in_dim(extended, (first + offset) * BLK, group_rows * BLK, 0)
            segment = shift_slots(segment, offset - H)
            stacked.append(segment.reshape(group_rows, BLK, S * BLK))
        gathered = jnp.stack(stacked, 1).reshape(group_rows, S * BLK, S * BLK).astype(jnp.float32)
        left_rows = lax.dynamic_slice_in_dim(left, first * BLK, group_rows * BLK, 0)
        left_rows = left_rows.reshape(group_rows, BLK, S * BLK).astype(jnp.float32)
        result = jnp.einsum("gak,gkn->gan", left_rows, gathered)
        return result.reshape(group_rows * BLK, S * BLK)

    result = lax.map(one_group, jnp.arange(NB // group_rows, dtype=jnp.int32))
    return result.reshape(NB * BLK, S * BLK)


def diagonal_sum(values):
    blocks = values.reshape(NB, BLK, S, BLK)[:, :, H, :]
    return jnp.sum(jnp.diagonal(blocks, axis1=1, axis2=2).astype(jnp.float32))


def reference(density, pattern, filter_mask):
    valid = valid_slots(NB, S, H)
    kept = expand_mask(density, pattern * valid)
    square = band_product(kept, kept)
    keep_filter = filter_mask * valid
    squared = expand_mask(square, keep_filter).astype(jnp.bfloat16)
    cube = band_product(squared, kept)
    purified = (3.0 * squared.astype(jnp.float32) - 2.0 * expand_mask(cube, keep_filter)).astype(jnp.bfloat16)
    traces = jnp.stack([diagonal_sum(kept), diagonal_sum(squared)]) / ORDER
    return purified, traces
```

```python
import functools

import jax
import jax.numpy as jnp
from jax import lax
from jax.experimental import pallas as pl
from jax.experimental.pallas import tpu as pltpu
from jax.sharding import PartitionSpec as P

BLK = 32
LANE = 128
PER = LANE // BLK
MESH = pl.DeviceIdType.MESH

RELAYED = ((1, 0, 4), (3, 0, 2), (3, 2, 2), (2, 0, 2), (2, 2, 2), (0, 0, 4))
DIRECT = (0, 1, 2)
ORDER = (1, 3, 2, 0)


def expander(width):
    row = lax.broadcasted_iota(jnp.int32, (LANE, width), 0)
    col = lax.broadcasted_iota(jnp.int32, (LANE, width), 1)
    return (col // BLK == row).astype(jnp.bfloat16)


def lanes_padded(value):
    short = LANE - value.shape[1]
    return jnp.concatenate([value, jnp.zeros((value.shape[0], short), value.dtype)], 1)


def valid_slots(first_row, rows, first_slot, half, total):
    row = lax.broadcasted_iota(jnp.int32, (rows, LANE), 0) + first_row
    slot = lax.broadcasted_iota(jnp.int32, (rows, LANE), 1) + first_slot
    column = row + slot - half
    return ((column >= 0) & (column < total)).astype(jnp.float32)


def kernel(
    row_size,
    density_in,
    pattern_in,
    filter_in,
    out,
    traces,
    density,
    pattern,
    filter_mask,
    spread,
    kept,
    far,
    opp,
    right,
    total_sum,
    squared,
    keep_filter,
    result,
    outbox,
    part,
    parts,
    load_sem,
    msend_sem,
    xsend_sem,
    m_sem,
    x_sem,
    rsend_sem,
    osend_sem,
    own_sem,
    fsend_sem,
    opp_sem,
    bsend_sem,
    box_sem,
    tsend_sem,
    trecv_sem,
    round_sem,
    done_sem,
):
    rows, width = density_in.shape
    half = width // BLK
    block_rows = rows // BLK
    mine = block_rows // 2
    groups = block_rows // PER
    group = PER * BLK
    tile = mine * BLK
    span = 5 * tile
    snap = lax.axis_index("snap")
    me = lax.axis_index("row")
    core = lax.axis_index("col")
    odd = lax.rem(me, 2)
    other = 1 - core
    partner = me + 1 - 2 * odd
    side = me - 1 + 2 * odd
    onward = me + 2 - 4 * odd
    origin = me - 2 + 4 * odd
    has_onward = (onward >= 0) & (onward < row_size)
    has_origin = (origin >= 0) & (origin < row_size)
    relays = core != odd
    has_far = relays | has_origin
    has_opp = (core == odd) | has_origin
    total = row_size * block_rows

    barrier = pltpu.get_barrier_semaphore()

    def greet(row, column, semaphore):
        pl.semaphore_signal(semaphore, inc=1, device_id=(snap, row, column), device_id_type=MESH)

    greet(me, other, barrier)
    greet(partner, core, barrier)
    greet(partner, other, barrier)

    @pl.when(has_onward)
    def _():
        greet(onward, core, barrier)
        greet(onward, other, barrier)

    @pl.when(has_origin)
    def _():
        greet(origin, core, barrier)
        greet(origin, other, barrier)
        greet(side, other, barrier)

    def band_of(flip, g):
        return pl.ds(pl.multiple_of((g + flip * (groups - 1 - 2 * g)) * group, group), group)

    loads = [pltpu.make_async_copy(pattern_in, pattern, load_sem.at[0])]
    for g in ORDER:
        at = band_of(core, g)
        loads.append(pltpu.make_async_copy(density_in.at[at, :], density.at[at, :], load_sem.at[1 + g]))
    loads.append(pltpu.make_async_copy(filter_in, filter_mask, load_sem.at[1 + groups]))
    for load in loads:
        load.start()

    def window(flip, row, height, slot, slots):
        row = row + flip * (block_rows - height - 2 * row)
        slot = slot + flip * (2 * half - slots - 2 * slot)
        return (
            pl.ds(pl.multiple_of(row * BLK, BLK), height * BLK),
            pl.ds(pl.multiple_of(slot * BLK, LANE), slots * BLK),
        )

    def relayed(flip, k):
        g, row, height = RELAYED[k]
        slots = PER * (g + 1)
        return window(flip, PER * g + row, height, half - slots, slots)

    def direct(flip, k):
        g = DIRECT[k]
        return window(flip, PER * g, PER, 0, half - PER * (g + 1))

    def send_relayed(j, k):
        at = relayed(j, k)
        return pltpu.make_async_remote_copy(
            src_ref=kept.at[at],
            dst_ref=far.at[at],
            send_sem=msend_sem.at[k],
            recv_sem=m_sem.at[j, k],
            device_id=(snap, partner, odd),
            device_id_type=MESH,
        )

    to_row = jnp.where(relays, partner, side)
    to_core = jnp.where(relays, odd, 1 - odd)

    def send_direct(j, k):
        at = direct(j, k)
        return pltpu.make_async_remote_copy(
            src_ref=kept.at[at],
            dst_ref=far.at[at],
            send_sem=xsend_sem.at[k],
            recv_sem=x_sem.at[k],
            device_id=(snap, to_row, to_core),
            device_id_type=MESH,
        )

    def relay(j, k):
        at = relayed(j, k)
        return pltpu.make_async_remote_copy(
            src_ref=far.at[at],
            dst_ref=far.at[at],
            send_sem=rsend_sem.at[j, k],
            recv_sem=m_sem.at[j, k],
            device_id=(snap, onward, odd),
            device_id_type=MESH,
        )

    def own_half(column, g):
        at = (band_of(column, g), pl.ds(pl.multiple_of(column * width, LANE), width))
        return pltpu.make_async_remote_copy(
            src_ref=kept.at[at],
            dst_ref=kept.at[at],
            send_sem=osend_sem.at[g],
            recv_sem=own_sem.at[g],
            device_id=(snap, me, other),
            device_id_type=MESH,
        )

    near_parts = (
        (groups - 2, half - PER, 3 * PER),
        (groups - 1, half - 2 * PER, 3 * PER),
        (groups - 1, half + PER, 3 * PER),
        (groups - 2, half + 2 * PER, 2 * PER),
    )

    def forward(column, n):
        g, slot, slots = near_parts[n]
        at = window(column, PER * g, PER, slot, slots)
        return pltpu.make_async_remote_copy(
            src_ref=far.at[at],
            dst_ref=opp.at[at],
            send_sem=fsend_sem.at[n],
            recv_sem=opp_sem.at[n],
            device_id=(snap, me, other),
            device_id_type=MESH,
        )

    loads[0].wait()
    keep = lanes_padded(pattern[...]).astype(jnp.float32)
    keep = keep * valid_slots(me * block_rows, block_rows, core * half, half, total)
    spread[...] = jnp.dot(keep.astype(jnp.bfloat16), expander(width), preferred_element_type=jnp.float32)
    own_lanes = pl.ds(pl.multiple_of(core * width, LANE), width)
    pieces = {1: (0,), 3: (1, 2), 2: (3, 4), 0: (5,)}
    for n, g in enumerate(ORDER):
        loads[1 + n].wait()
        first = g + core * (groups - 1 - 2 * g)
        for r in range(PER):
            m = first * PER + r
            at = pl.ds(pl.multiple_of(m * BLK, BLK), BLK)
            kept[at, own_lanes] = (density[at, :].astype(jnp.float32) * spread[pl.ds(m, 1), :]).astype(jnp.bfloat16)
        if n == 0:
            beside = 2 * has_onward.astype(jnp.int32) + 3 * has_origin.astype(jnp.int32)
            pl.semaphore_wait(barrier, 3 + beside)
        for k in pieces[g]:
            send_relayed(core, k).start()
        own_half(core, g).start()

    @pl.when(has_far)
    def _():
        for k in range(len(DIRECT)):
            send_direct(core, k).start()

    levels = max(row_size // 2, 1)

    def meet(level):
        @pl.when(has_onward)
        def _():
            greet(onward, core, round_sem.at[level])

        @pl.when(has_origin)
        def _():
            greet(origin, core, round_sem.at[level])

    def met(level):
        pl.semaphore_wait(round_sem.at[level], has_onward.astype(jnp.int32) + has_origin.astype(jnp.int32))

    def round_of(level):
        if 1 <= level - 1 < levels:
            met(level - 1)
        if 1 <= level < levels:
            meet(level)

    round_of(1)
    loads[-1].wait()
    keep = lanes_padded(filter_mask[pl.ds(pl.multiple_of(core * mine, mine), mine), :]).astype(jnp.float32)
    keep = keep * valid_slots(me * block_rows + core * mine, mine, 0, half, total)
    keep = pltpu.roll(keep, 0, 1, stride=1, stride_axis=0)
    keep_filter[...] = jnp.dot(keep.astype(jnp.bfloat16), expander(span), preferred_element_type=jnp.float32)
    right[:, pl.ds(width, span)] = jnp.zeros((span, span), right.dtype)

    def lay(source, first, place):
        for r in range(PER):
            at = pl.ds(pl.multiple_of((first + r) * BLK, BLK), BLK)
            band = jnp.concatenate([source[at, :], jnp.zeros((BLK, LANE), jnp.bfloat16)], 1)
            if r:
                band = pltpu.roll(band.astype(jnp.float32), r * BLK, 1).astype(jnp.bfloat16)
            to = pl.ds(pl.multiple_of((place + r) * BLK, BLK), BLK)
            right[to, pl.ds(pl.multiple_of(place * BLK, LANE), 2 * width + LANE)] = band

    def lay_own(g):
        first = (g + other * (groups - 1 - 2 * g)) * PER
        lay(kept, first, 2 * mine - core * mine + first)

    def lay_far(g):
        first = (g + core * (groups - 1 - 2 * g)) * PER
        lay(far, first, first + core * 3 * mine)

    def lay_opp(g):
        first = (g + other * (groups - 1 - 2 * g)) * PER
        lay(opp, first, first + other * 4 * mine - core * mine)

    def tiles(first, count):
        first = first + core * (5 - count - 2 * first)
        return pl.multiple_of(first * tile, tile)

    def product(k, depth, first, count, add):
        here = tiles(k, depth)
        there = tiles(first, count)
        value = jnp.dot(
            right[pl.ds(2 * tile, tile), pl.ds(pl.multiple_of(width + here, LANE), depth * tile)],
            right[pl.ds(here, depth * tile), pl.ds(pl.multiple_of(width + there, LANE), count * tile)],
            preferred_element_type=jnp.float32,
        )
        if add:
            total_sum[:, pl.ds(there, count * tile)] += value
        else:
            total_sum[:, pl.ds(there, count * tile)] = value

    def arrive(k):
        @pl.when(has_far)
        def _():
            for j in range(2):
                relay(j, k).wait_recv()

        @pl.when(relays & has_onward)
        def _():
            for j in range(2):
                relay(j, k).start()

    def pass_on(n):
        @pl.when(has_far)
        def _():
            forward(core, n).start()

    def arrive_direct(k):
        @pl.when(has_far)
        def _():
            send_direct(other, k).wait_recv()

    for g in ORDER:
        own_half(other, g).wait_recv()
        lay_own(g)
    arrive(0)
    round_of(2)
    product(2, 2, 0, 5, False)
    arrive(1)
    arrive(2)
    round_of(3)
    arrive(3)
    arrive(4)
    pass_on(0)
    round_of(4)
    arrive(5)
    pass_on(1)

    @pl.when(has_far)
    def _():
        lay_far(0)

    for level in range(5, min(levels, 6) + 1):
        round_of(level)
    if levels > 5:

        def again(level, _):
            met(level - 1)
            meet(level)
            return 0

        lax.fori_loop(7, levels, again, 0)
        met(levels - 1)
    greet(me, other, done_sem)
    greet(partner, core, done_sem)
    greet(partner, other, done_sem)

    arrive_direct(0)
    pass_on(2)

    @pl.when(has_far)
    def _():
        lay_far(3)

    arrive_direct(1)
    pass_on(3)

    @pl.when(has_far)
    def _():
        lay_far(2)
        product(1, 1, 0, 4, True)

    def take_far():
        @pl.when(has_far)
        def _():
            send_direct(other, 2).wait_recv()
            lay_far(1)
            product(0, 1, 0, 3, True)

    def take_opp():
        @pl.when(has_opp)
        def _():
            for n in (1, 2):
                forward(other, n).wait_recv()
            lay_opp(groups - 1)
            for n in (0, 3):
                forward(other, n).wait_recv()
            lay_opp(groups - 2)
            product(4, 1, 2, 3, True)

    @pl.when(relays)
    def _():
        take_far()
        take_opp()

    @pl.when(core == odd)
    def _():
        take_opp()
        take_far()

    pl.semaphore_wait(done_sem, 3)

    lane = lax.broadcasted_iota(jnp.int32, (LANE, LANE), 1)
    diagonal = lane == lax.broadcasted_iota(jnp.int32, (LANE, LANE), 0)
    kept_sum = jnp.zeros((LANE, LANE), jnp.float32)
    squared_sum = jnp.zeros((LANE, LANE), jnp.float32)
    for b in range(tile // LANE):
        here = pl.ds(2 * tile + b * LANE, LANE)
        kept_sum += jnp.where(diagonal, right[here, pl.ds(width + 2 * tile + b * LANE, LANE)].astype(jnp.float32), 0.0)
        blocks = []
        for m in range(b * PER, (b + 1) * PER):
            blocks.append(total_sum[pl.ds(m * BLK, BLK), here] * keep_filter[pl.ds(m, 1), here])
        squared_sum += jnp.where(diagonal, jnp.concatenate(blocks, 0).astype(jnp.bfloat16).astype(jnp.float32), 0.0)
    part[0] = jnp.sum(kept_sum.reshape(LANE // 8, 8, LANE), 0)
    part[1] = jnp.sum(squared_sum.reshape(LANE // 8, 8, LANE), 0)

    number = 2 * me + core

    def share(step, peer):
        return pltpu.make_async_remote_copy(
            src_ref=part,
            dst_ref=parts.at[step],
            send_sem=tsend_sem.at[step],
            recv_sem=trecv_sem.at[step],
            device_id=(snap, peer // 2, lax.rem(peer, 2)),
            device_id_type=MESH,
        )

    def give(step, _):
        share(step, lax.rem(number + step, 2 * row_size)).start()
        return 0

    lax.fori_loop(1, 2 * row_size, give, 0)

    for m in range(mine):
        at = pl.ds(m * BLK, BLK)
        squared[at, :] = (total_sum[at, :] * keep_filter[m : m + 1, :]).astype(jnp.bfloat16)

    def cube(first, low, depth):
        there = pl.ds(tiles(first, 1), tile)
        here = pl.ds(tiles(low, depth), depth * tile)
        value = jnp.dot(
            squared[:, here],
            right[here, pl.ds(pl.multiple_of(width + tiles(first, 1), LANE), tile)],
            preferred_element_type=jnp.float32,
        )
        for m in range(mine):
            at = pl.ds(m * BLK, BLK)
            result[at, there] = 3.0 * squared[at, there].astype(jnp.float32) - 2.0 * (
                value[m * BLK : (m + 1) * BLK] * keep_filter[pl.ds(m, 1), there]
            )

    def unskewed(m, column):
        turn = (m % PER) * BLK
        start = pl.multiple_of(column * width + m * BLK - turn, LANE)
        band = result[pl.ds(m * BLK, BLK), pl.ds(start, width + (LANE if turn else 0))]
        if turn:
            band = pltpu.roll(band, band.shape[1] - turn, 1)
        return band[:, :width].astype(jnp.bfloat16)

    def box(column, n):
        here = pl.ds(n * group, group)
        there = pl.ds(pl.multiple_of(column * tile + n * group, group), group)
        return pltpu.make_async_remote_copy(
            src_ref=outbox.at[here, :],
            dst_ref=out.at[there, :],
            send_sem=bsend_sem.at[n],
            recv_sem=box_sem.at[n],
            device_id=(snap, me, other),
            device_id_type=MESH,
        )

    cube(4, 2, 3)
    cube(3, 1, 4)
    cube(2, 0, 5)
    for m in range(mine):
        outbox[pl.ds(m * BLK, BLK), :] = unskewed(m, other)
        if m % PER == PER - 1:
            box(core, m // PER).start()
    cube(1, 0, 4)
    cube(0, 0, 3)
    for m in range(mine):
        at = pl.ds(pl.multiple_of(core * tile + m * BLK, BLK), BLK)
        out[at, :] = unskewed(m, core)

    def gather(step, sums):
        share(step, lax.rem(number + 2 * row_size - step, 2 * row_size)).wait()
        return (sums[0] + parts[step, 0], sums[1] + parts[step, 1])

    sums = lax.fori_loop(1, 2 * row_size, gather, (part[0], part[1]))
    traces[0] = jnp.sum(sums[0]) / (total * BLK)
    traces[1] = jnp.sum(sums[1]) / (total * BLK)

    for n in range(tile // group):
        box(core, n).wait_send()
        box(other, n).wait_recv()
    for g in range(groups):
        own_half(core, g).wait_send()
    for k in range(len(RELAYED)):
        send_relayed(core, k).wait_send()

        @pl.when(relays & has_onward)
        def _():
            for j in range(2):
                relay(j, k).wait_send()

    @pl.when(has_far)
    def _():
        for k in range(len(DIRECT)):
            send_direct(core, k).wait_send()
        for n in range(len(near_parts)):
            forward(core, n).wait_send()


def solution(mesh):
    row_size = mesh.shape["row"]

    def per_device(density, pattern, filter_mask):
        rows, width = density.shape
        block_rows = rows // BLK
        tile = rows // 2
        span = 5 * tile
        dma = pltpu.SemaphoreType.DMA
        return pl.pallas_call(
            functools.partial(kernel, row_size),
            out_shape=(
                pltpu.VMEM((rows, width), jnp.bfloat16),
                jax.ShapeDtypeStruct((2,), jnp.float32),
            ),
            in_specs=[pl.BlockSpec(memory_space=pl.ANY)] * 3,
            out_specs=(
                pl.BlockSpec(memory_space=pltpu.VMEM),
                pl.BlockSpec(memory_space=pltpu.SMEM),
            ),
            scratch_shapes=[
                pltpu.VMEM((rows, width), jnp.bfloat16),
                pltpu.VMEM(pattern.shape, jnp.int32),
                pltpu.VMEM(filter_mask.shape, jnp.int32),
                pltpu.VMEM((block_rows, width), jnp.float32),
                pltpu.VMEM((rows, 2 * width), jnp.bfloat16),
                pltpu.VMEM((rows, 2 * width), jnp.bfloat16),
                pltpu.VMEM((rows, 2 * width), jnp.bfloat16),
                pltpu.VMEM((span, span + 2 * width), jnp.bfloat16),
                pltpu.VMEM((tile, span), jnp.float32),
                pltpu.VMEM((tile, span), jnp.bfloat16),
                pltpu.VMEM((block_rows // 2, span), jnp.float32),
                pltpu.VMEM((tile, span), jnp.float32),
                pltpu.VMEM((tile, width), jnp.bfloat16),
                pltpu.VMEM((2, 8, LANE), jnp.float32),
                pltpu.VMEM((2 * row_size, 2, 8, LANE), jnp.float32),
                dma((2 + block_rows // PER,)),
                dma((len(RELAYED),)),
                dma((len(DIRECT),)),
                dma((2, len(RELAYED))),
                dma((len(DIRECT),)),
                dma((2, len(RELAYED))),
                dma((block_rows // PER,)),
                dma((block_rows // PER,)),
                dma((4,)),
                dma((4,)),
                dma((2,)),
                dma((2,)),
                dma((2 * row_size,)),
                dma((2 * row_size,)),
                pltpu.SemaphoreType.REGULAR((max(row_size // 2, 1),)),
                pltpu.SemaphoreType.REGULAR,
            ],
            compiler_params=pltpu.CompilerParams(
                collective_id=0, has_side_effects=True, vmem_limit_bytes=56 * 1024 * 1024
            ),
        )(density, pattern, filter_mask)

    return jax.shard_map(
        per_device,
        mesh=mesh,
        in_specs=(P(("snap", "row"), "col"), P(("snap", "row"), "col"), P(("snap", "row"), None)),
        out_specs=(P(("snap", "row"), "col"), P("snap")),
        check_vma=False,
    )
```
